8 devices in a mesh: dp: 2 (over y, z), ep: 4 (over x, core).
Axes of the slice: x: 2, y: 2, z: 1, core: 2. Of those that a mesh axis runs over, the one named last changes fastest.
Arguments:
- x: bfloat16 [2, 4, 512, 4096], P('dp', 'ep'), parts along dimension 0
- expert: int32 [2, 4, 512, 2], P('dp', 'ep'), parts along dimension 0
- slot: int32 [2, 4, 512, 2], P('dp', 'ep'), parts along dimension 0
- gate: float32 [2, 4, 512, 2], P('dp', 'ep'), parts along dimension 0
- w_gate: bfloat16 [16, 4096, 6400], P('ep')
- w_up: bfloat16 [16, 4096, 6400], P('ep')
- w_down: bfloat16 [16, 6400, 4096], P('ep')
Outputs:
- y: bfloat16 [2, 4, 512, 4096], P('dp', 'ep'), parts along dimension 0
There are 2 independent parts. The reference program is written for one: setup_inputs(seed, part) draws one part's arguments, and reference() takes and returns one part's arrays. A program takes and returns all parts, laid end to end along the dimension named above; an argument that names none is the same for every part.
All inputs are finite; a program needn't handle non-finite values.
Results may differ from the reference program's by a relative error of at most 0.009.
Values are sent between devices in bfloat16 or wider.
A program may use at most 2 GiB of HBM per device.

```python
import jax
import jax.numpy as jnp

MEMBERS = 4
TOKENS = 512
D = 4096
FF = 6400
TOP = 2
EXPERTS = 16
SLOTS = 5 * TOKENS * TOP // (4 * EXPERTS)


def setup_inputs(seed: int = 0, part: int = 0) -> dict:
    own, k1, k2, k3, k4, k5, k6 = jax.random.split(jax.random.key(seed), 7)
    kx, ke, kl, kg = jax.random.split(jax.random.fold_in(own, part), 4)
    devices = (1, MEMBERS)
    place = jax.random.permutation(kl, jnp.arange(EXPERTS, dtype=jnp.uint32))
    slow = ((EXPERTS + (9 * place) % EXPERTS) << ((9 * place) // EXPERTS)) // EXPERTS
    wait = (jax.random.bits(ke, (*devices, TOKENS, EXPERTS), jnp.uint32) >> 10) * slow
    expert = jnp.argsort(wait, axis=-1)[..., :TOP].astype(jnp.int32)
    chosen = jax.nn.one_hot(expert, EXPERTS, dtype=jnp.int32)
    in_line = jnp.cumsum(chosen.reshape(*devices, TOKENS * TOP, EXPERTS), axis=2) - 1
    slot = jnp.sum(in_line.reshape(chosen.shape) * chosen, axis=-1)

    def one(key, rows, columns):
        return (jax.random.normal(key, (rows, columns), jnp.float32) * rows**-0.5).astype(jnp.bfloat16)

    def weights(key, rows, columns):
        return jax.lax.map(lambda k: one(k, rows, columns), jax.random.split(key, EXPERTS))

    return {
        "x": jax.random.normal(kx, (*devices, TOKENS, D), jnp.float32).astype(jnp.bfloat16),
        "expert": expert,
        "slot": slot,
        "gate": jax.nn.softmax(jax.random.normal(kg, expert.shape, jnp.float32)),
        "w_gate": weights(k1, D, FF),
        "w_up": weights(k2, D, FF),
        "w_down": weights(k3, FF, D),
    }


def einsum(form, a, b):
    return jnp.einsum(form, a.astype(jnp.float32), b.astype(jnp.float32))


def reference(x, expert, slot, gate, w_gate, w_up, w_down):
    to_expert = jax.nn.one_hot(expert, EXPERTS, dtype=jnp.bfloat16)
    to_slot = jax.nn.one_hot(slot, SLOTS, dtype=jnp.bfloat16)
    weighted = to_expert * gate[..., None].astype(jnp.bfloat16)
    dispatch = einsum("abtke,abtkc->abtec", to_expert, to_slot).astype(jnp.bfloat16)
    combine = einsum("abtke,abtkc->abtec", weighted, to_slot).astype(jnp.bfloat16)
    z = einsum("abtec,abtd->aebcd", dispatch, x).astype(jnp.bfloat16)
    h = jax.nn.silu(einsum("aebcd,edf->aebcf", z, w_gate))
    h = (h * einsum("aebcd,edf->aebcf", z, w_up)).astype(jnp.bfloat16)
    out = einsum("aebcf,efd->aebcd", h, w_down).astype(jnp.bfloat16)
    y = einsum("abtec,aebcd->abtd", combine, out)
    return y.astype(jnp.bfloat16)
```

```python
import functools

import jax
import jax.numpy as jnp
from jax import lax
from jax.experimental import pallas as pl
from jax.experimental.pallas import tpu as pltpu
from jax.sharding import PartitionSpec as P

MESH = pl.DeviceIdType.MESH
FT, DT, RING = 256, 512, 4


def einsum(form, a, b):
    return jnp.einsum(form, a.astype(jnp.float32), b.astype(jnp.float32))


def ffn_kernel(s_ref, wg, wu, wd, r_ref, z, h, o, ring, w_sem, z_send, z_recv, z_own, o_send, o_recv, o_own):
    members, experts, slots, d = s_ref.shape
    f = wg.shape[2]
    n1, n2 = f // FT, d // DT
    steps = n1 + n2
    me = lax.axis_index("ep")
    group = lax.axis_index("dp")

    def peer(k):
        return me ^ k

    def rows(i):
        return pl.ds(pl.multiple_of(i * slots, slots), slots)

    def w_issue(g):
        e, s, at = g // steps, lax.rem(g, steps), lax.rem(g, RING)

        @pl.when(s < n1)
        def _():
            c = pl.ds(pl.multiple_of(s * FT, FT), FT)
            for j, w in enumerate((wg, wu)):
                pltpu.make_async_copy(
                    w.at[e, :, c], ring.at[at, pl.ds(0, d), pl.ds(j * FT, FT)], w_sem.at[at, j]
                ).start()

        @pl.when(s >= n1)
        def _():
            c = pl.ds(pl.multiple_of((s - n1) * DT, DT), DT)
            pltpu.make_async_copy(wd.at[e, :, c], ring.at[at], w_sem.at[at, 0]).start()

    def z_copy(e, k):
        return pltpu.make_async_remote_copy(
            s_ref.at[peer(k), e], z.at[e, rows(me)], z_send.at[e, k - 1], z_recv.at[e, k - 1],
            device_id=(group, peer(k)), device_id_type=MESH,
        )

    def z_arrival(e, k):
        return pltpu.make_async_remote_copy(
            s_ref.at[peer(k), e], z.at[e, rows(peer(k))], z_send.at[e, k - 1], z_recv.at[e, k - 1],
            device_id=(group, peer(k)), device_id_type=MESH,
        )

    def z_local(e):
        return pltpu.make_async_copy(s_ref.at[me, e], z.at[e, rows(me)], z_own.at[e])

    def o_copy(e, s, k):
        c = pl.ds(pl.multiple_of(s * DT, DT), DT)
        return pltpu.make_async_remote_copy(
            o.at[lax.rem(e, 2), rows(peer(k)), c], r_ref.at[me, e, :, c], o_send.at[e, s, k - 1],
            o_recv.at[e, s, k - 1], device_id=(group, peer(k)), device_id_type=MESH,
        )

    def o_arrival(e, s, k):
        c = pl.ds(pl.multiple_of(s * DT, DT), DT)
        return pltpu.make_async_remote_copy(
            o.at[lax.rem(e, 2), rows(me), c], r_ref.at[peer(k), e, :, c], o_send.at[e, s, k - 1],
            o_recv.at[e, s, k - 1], device_id=(group, peer(k)), device_id_type=MESH,
        )

    def o_local(e, s):
        c = pl.ds(pl.multiple_of(s * DT, DT), DT)
        return pltpu.make_async_copy(o.at[lax.rem(e, 2), rows(me), c], r_ref.at[me, e, :, c], o_own.at[e, s])

    for g in range(RING - 1):
        w_issue(g)
    barrier = pltpu.get_barrier_semaphore()
    for k in (1, 2, 3):
        pl.semaphore_signal(barrier, inc=1, device_id=(group, peer(k)), device_id_type=MESH)
    pl.semaphore_wait(barrier, 3)
    for e in range(experts):
        for k in (2, 3, 1):
            z_copy(e, k).start()
        z_local(e).start()

    def give_back(e, s):
        for k in (2, 3, 1):
            o_copy(e, s, k).start()
        o_local(e, s).start()

    def given(e):
        def one(s, _):
            for k in (1, 2, 3):
                o_copy(e, s, k).wait_send()
            o_local(e, s).wait()
            return 0

        lax.fori_loop(0, n2, one, 0)

    def expert(e, _):
        for k in (1, 2, 3):
            z_arrival(e, k).wait_recv()
        z_local(e).wait()

        def up(s, _):
            g = e * steps + s
            at = lax.rem(g, RING)

            @pl.when(g + RING - 1 < experts * steps)
            def _():
                w_issue(g + RING - 1)

            for j, w in enumerate((wg, wu)):
                pltpu.make_async_copy(
                    w.at[0, :, pl.ds(0, FT)], ring.at[at, pl.ds(0, d), pl.ds(j * FT, FT)], w_sem.at[at, j]
                ).wait()
            both = jnp.dot(z[e], ring[at, :d, :], preferred_element_type=jnp.float32)
            a, b = both[:, :FT], both[:, FT:]
            h[:, pl.ds(pl.multiple_of(s * FT, FT), FT)] = (jax.nn.silu(a) * b).astype(h.dtype)
            return 0

        lax.fori_loop(0, n1, up, 0)

        @pl.when(e >= 2)
        def _():
            given(e - 2)

        def down(s, _):
            g = e * steps + n1 + s
            at = lax.rem(g, RING)

            @pl.when(g + RING - 1 < experts * steps)
            def _():
                w_issue(g + RING - 1)

            pltpu.make_async_copy(wd.at[0, :, pl.ds(0, DT)], ring.at[at], w_sem.at[at, 0]).wait()

            @pl.when(s >= 1)
            def _():
                give_back(e, s - 1)

            c = pl.ds(pl.multiple_of(s * DT, DT), DT)
            o[lax.rem(e, 2), :, c] = jnp.dot(h[...], ring[at], preferred_element_type=jnp.float32).astype(o.dtype)
            return 0

        lax.fori_loop(0, n2, down, 0)
        give_back(e, n2 - 1)
        return 0

    lax.fori_loop(0, experts, expert, 0)
    given(experts - 2)
    given(experts - 1)

    def last(e, _):
        for k in (1, 2, 3):
            z_copy(e, k).wait_send()

        def one(s, _):
            for k in (1, 2, 3):
                o_arrival(e, s, k).wait_recv()
            return 0

        return lax.fori_loop(0, n2, one, 0)

    lax.fori_loop(0, experts, last, 0)


def moe(s, wg, wu, wd):
    members, experts, slots, d = s.shape
    f = wg.shape[2]
    n2 = d // DT
    dma, rows = pltpu.SemaphoreType.DMA, members * slots
    return pl.pallas_call(
        ffn_kernel,
        out_shape=jax.ShapeDtypeStruct(s.shape, s.dtype),
        in_specs=[pl.BlockSpec(memory_space=pl.ANY)] * 4,
        out_specs=pl.BlockSpec(memory_space=pl.ANY),
        scratch_shapes=[
            pltpu.VMEM((experts, rows, d), s.dtype),
            pltpu.VMEM((rows, f), s.dtype),
            pltpu.VMEM((2, rows, d), s.dtype),
            pltpu.VMEM((RING, f, 2 * FT), s.dtype),
            dma((RING, 2)),
            dma((experts, 3)),
            dma((experts, 3)),
            dma((experts,)),
            dma((experts, n2, 3)),
            dma((experts, n2, 3)),
            dma((experts, n2)),
        ],
        compiler_params=pltpu.CompilerParams(
            collective_id=0, has_side_effects=True, vmem_limit_bytes=60 * 2**20
        ),
    )(s, wg, wu, wd)


def solution(mesh):
    members = mesh.shape["ep"]

    def step(x, expert, slot, gate, w_gate, w_up, w_down):
        x, expert, slot, gate = x[0, 0], expert[0, 0], slot[0, 0], gate[0, 0]
        (tokens, top), experts, d = expert.shape, members * w_gate.shape[0], x.shape[1]
        slots = 5 * tokens * top // (4 * experts)
        to_expert = jax.nn.one_hot(expert, experts, dtype=jnp.bfloat16)
        to_slot = jax.nn.one_hot(slot, slots, dtype=jnp.bfloat16)
        weighted = to_expert * gate[..., None].astype(jnp.bfloat16)
        dispatch = einsum("tke,tkc->tec", to_expert, to_slot).astype(jnp.bfloat16)
        combine = einsum("tke,tkc->tec", weighted, to_slot).astype(jnp.bfloat16)
        s = einsum("tec,td->ecd", dispatch, x).astype(jnp.bfloat16)
        s = s.reshape(members, experts // members, slots, d)
        r = moe(s, w_gate, w_up, w_down).reshape(experts, slots, d)
        y = einsum("tec,ecd->td", combine, r)
        return y.astype(jnp.bfloat16)[None, None]

    own, weights = P("dp", "ep"), P("ep")
    return jax.shard_map(
        step, mesh=mesh, in_specs=(own, own, own, own, weights, weights, weights), out_specs=own, check_vma=False
    )
```

```python
import functools

import jax
import jax.numpy as jnp
from jax import lax
from jax.experimental import pallas as pl
from jax.experimental.pallas import tpu as pltpu
from jax.sharding import PartitionSpec as P

MESH = pl.DeviceIdType.MESH
FT, DT, RING, PAIR = 256, 512, 5, 2
AHEAD = RING - PAIR


def cell_of(expert_ref, slot_ref, slots):
    slot = slot_ref[...]
    return jnp.where(slot < slots, expert_ref[...] * slots + slot, -1)


def ffn_kernel(
    expert_ref, slot_ref, x_ref, wg, wu, wd, r_ref, sent, z, h, o, ring,
    x_sem, w_sem, z_send, z_recv, o_send, o_recv, o_own,
):
    experts, rows_z, d = z.shape
    members = r_ref.shape[0]
    slots = rows_z // members
    tokens, f = x_ref.shape[0], wg.shape[2]
    n1, n2 = f // FT, d // DT
    steps, total, back = n1 + n2, experts * (n1 + n2), n2 // PAIR
    me, group = lax.axis_index("ep"), lax.axis_index("dp")

    def peer(k):
        return me ^ k

    def rows(i):
        return pl.ds(pl.multiple_of(i * slots, slots), slots)

    def x_copy(j):
        return pltpu.make_async_copy(
            x_ref.at[:, pl.ds(j * DT, DT)], ring.at[RING - 1, pl.ds(j * tokens, tokens)], x_sem.at[j]
        )

    def w_issue(g):
        e, s, at = g // steps, lax.rem(g, steps), lax.rem(g, RING)

        @pl.when((s < n1) & (g < total))
        def _():
            c = pl.ds(pl.multiple_of(s * FT, FT), FT)
            for j, w in enumerate((wg, wu)):
                pltpu.make_async_copy(
                    w.at[e, :, c], ring.at[at, pl.ds(0, d), pl.ds(j * FT, FT)], w_sem.at[at, j]
                ).start()

        @pl.when((s >= n1) & (g < total))
        def _():
            c = pl.ds(pl.multiple_of((s - n1) * DT, DT), DT)
            pltpu.make_async_copy(wd.at[e, :, c], ring.at[at], w_sem.at[at, 0]).start()

    def z_copy(e, k):
        return pltpu.make_async_remote_copy(
            sent.at[e, pl.ds((k - 1) * slots, slots)], z.at[e, rows(me)], z_send.at[e, k - 1], z_recv.at[e, k - 1],
            device_id=(group, peer(k)), device_id_type=MESH,
        )

    def z_arrival(e, k):
        return pltpu.make_async_remote_copy(
            sent.at[e, pl.ds((k - 1) * slots, slots)], z.at[e, rows(peer(k))], z_send.at[e, k - 1],
            z_recv.at[e, k - 1], device_id=(group, peer(k)), device_id_type=MESH,
        )

    def back_columns(s):
        return pl.ds(pl.multiple_of(s * (PAIR * DT), PAIR * DT), PAIR * DT)

    def o_copy(e, s, k):
        c = back_columns(s)
        return pltpu.make_async_remote_copy(
            o.at[lax.rem(e, 2), rows(peer(k)), c], r_ref.at[me, e, :, c], o_send.at[e, s, k - 1],
            o_recv.at[e, s, k - 1], device_id=(group, peer(k)), device_id_type=MESH,
        )

    def o_arrival(e, s, k):
        c = back_columns(s)
        return pltpu.make_async_remote_copy(
            o.at[lax.rem(e, 2), rows(me), c], r_ref.at[peer(k), e, :, c], o_send.at[e, s, k - 1],
            o_recv.at[e, s, k - 1], device_id=(group, peer(k)), device_id_type=MESH,
        )

    def o_local(e, s):
        c = back_columns(s)
        return pltpu.make_async_copy(o.at[lax.rem(e, 2), rows(me), c], r_ref.at[me, e, :, c], o_own.at[e, s])

    for j in range(n2):
        x_copy(j).start()
    barrier = pltpu.get_barrier_semaphore()
    for k in (1, 2, 3):
        pl.semaphore_signal(barrier, inc=1, device_id=(group, peer(k)), device_id_type=MESH)
    for g in range(AHEAD):
        w_issue(jnp.int32(g))

    cell = cell_of(expert_ref, slot_ref, slots)
    row = lax.broadcasted_iota(jnp.int32, (rows_z, tokens), 0)
    k_of = sum((row >= i * slots).astype(jnp.int32) for i in range(1, members))
    first = (me ^ k_of) * (experts * slots) + row - k_of * slots
    for j in range(n2):
        x_copy(j).wait()
    pl.semaphore_wait(barrier, 3)

    def send(e):
        for k in (2, 3, 1):
            z_copy(e, k).start()

    def dispatch(e, _):
        want = first + e * slots
        hot = ((cell[0:1] == want) | (cell[1:2] == want)).astype(jnp.float32).astype(z.dtype)

        def part(i, _):
            for j in range(PAIR):
                c = i * PAIR + j
                block = ring[RING - 1, pl.ds(pl.multiple_of(c * tokens, tokens), tokens), :]
                v = jnp.dot(hot, block, preferred_element_type=jnp.float32).astype(z.dtype)
                cols = pl.ds(pl.multiple_of(c * DT, DT), DT)
                z[e, rows(me), cols] = v[:slots]
                sent[e, :, cols] = v[slots:]

            @pl.when((i == 0) & (e > 0))
            def _():
                send(e - 1)

            return 0

        return lax.fori_loop(0, back, part, 0)

    lax.fori_loop(0, experts, dispatch, 0)

    def give_back(e, s):
        for k in (2, 3, 1):
            o_copy(e, s, k).start()
        o_local(e, s).start()

    def given(e):
        def one(s, _):
            for k in (1, 2, 3):
                o_copy(e, s, k).wait_send()
            o_local(e, s).wait()
            return 0

        lax.fori_loop(0, back, one, 0)

    def up(e, s, n):
        g = e * steps + s
        for i in range(n):
            w_issue(g + AHEAD + i)
        for i in range(n):
            at = lax.rem(g + i, RING)
            for j, w in enumerate((wg, wu)):
                pltpu.make_async_copy(
                    w.at[0, :, pl.ds(0, FT)], ring.at[at, pl.ds(0, d), pl.ds(j * FT, FT)], w_sem.at[at, j]
                ).wait()
        for i in range(n):
            both = jnp.dot(z[e], ring[lax.rem(g + i, RING), :d, :], preferred_element_type=jnp.float32)
            a, b = both[:, :FT], both[:, FT:]
            h[:, pl.ds(pl.multiple_of((s + i) * FT, FT), FT)] = (jax.nn.silu(a) * b).astype(h.dtype)

    def down(e, s, n):
        g = e * steps + n1 + s
        for i in range(n):
            w_issue(g + AHEAD + i)
        for i in range(n):
            at = lax.rem(g + i, RING)
            pltpu.make_async_copy(wd.at[0, :, pl.ds(0, DT)], ring.at[at], w_sem.at[at, 0]).wait()

        @pl.when(s > 0)
        def _():
            give_back(e, s // PAIR - 1)

        for i in range(n):
            c = pl.ds(pl.multiple_of((s + i) * DT, DT), DT)
            o[lax.rem(e, 2), :, c] = jnp.dot(
                h[...], ring[lax.rem(g + i, RING)], preferred_element_type=jnp.float32
            ).astype(o.dtype)

    def in_pairs(step, e, n):
        def one(i, _):
            step(e, i * PAIR, PAIR)
            return 0

        lax.fori_loop(0, n // PAIR, one, 0)
        if n % PAIR:
            step(e, n - n % PAIR, n % PAIR)

    def expert(e, _):
        for k in (1, 2, 3):
            z_arrival(e, k).wait_recv()

        @pl.when(e == 0)
        def _():
            send(experts - 1)

        @pl.when(e > 0)
        def _():
            give_back(e - 1, back - 1)

        in_pairs(up, e, n1)

        @pl.when(e >= 2)
        def _():
            given(e - 2)

        in_pairs(down, e, n2)
        return 0

    lax.fori_loop(0, experts, expert, 0)
    given(experts - 2)
    give_back(experts - 1, back - 1)
    given(experts - 1)

    def last(e, _):
        for k in (1, 2, 3):
            z_copy(e, k).wait_send()

        def one(s, _):
            for k in (1, 2, 3):
                o_arrival(e, s, k).wait_recv()
            return 0

        return lax.fori_loop(0, back, one, 0)

    lax.fori_loop(0, experts, last, 0)


def moe(expert, slot, x, wg, wu, wd, members, slots):
    experts, d, f = wg.shape
    back, dma, rows = d // (DT * PAIR), pltpu.SemaphoreType.DMA, members * slots
    vmem, anywhere = pl.BlockSpec(memory_space=pltpu.VMEM), pl.BlockSpec(memory_space=pl.ANY)
    return pl.pallas_call(
        ffn_kernel,
        out_shape=jax.ShapeDtypeStruct((members, experts, slots, d), x.dtype),
        in_specs=[vmem, vmem] + [anywhere] * 4,
        out_specs=anywhere,
        scratch_shapes=[
            pltpu.VMEM((experts, rows - slots, d), x.dtype),
            pltpu.VMEM((experts, rows, d), x.dtype),
            pltpu.VMEM((rows, f), x.dtype),
            pltpu.VMEM((2, rows, d), x.dtype),
            pltpu.VMEM((RING, f, 2 * FT), x.dtype),
            dma((d // DT,)),
            dma((RING, 2)),
            dma((experts, 3)),
            dma((experts, 3)),
            dma((experts, back, 3)),
            dma((experts, back, 3)),
            dma((experts, back)),
        ],
        compiler_params=pltpu.CompilerParams(
            collective_id=0, has_side_effects=True, vmem_limit_bytes=67_000_000
        ),
    )(expert, slot, x, wg, wu, wd)


def combine_kernel(expert_ref, slot_ref, gate_ref, r_ref, y_ref, weights, *, slots):
    @pl.when(pl.program_id(0) == 0)
    def _():
        cell, gate = cell_of(expert_ref, slot_ref, slots), gate_ref[...].astype(jnp.bfloat16).astype(jnp.float32)
        q = lax.broadcasted_iota(jnp.int32, (r_ref.shape[0], cell.shape[1]), 0)
        w = sum(jnp.where(cell[j : j + 1] == q, gate[j : j + 1], 0.0) for j in range(cell.shape[0]))
        weights[...] = w.T.astype(jnp.bfloat16)

    y_ref[...] = jnp.dot(weights[...], r_ref[...], preferred_element_type=jnp.float32).astype(y_ref.dtype)


def combine(expert, slot, gate, r, slots):
    (top, tokens), (cells, d), width = expert.shape, r.shape, 512
    small = pl.BlockSpec((top, tokens), lambda i: (0, 0))
    return pl.pallas_call(
        functools.partial(combine_kernel, slots=slots),
        out_shape=jax.ShapeDtypeStruct((tokens, d), jnp.bfloat16),
        grid=(d // width,),
        in_specs=[small, small, small, pl.BlockSpec((cells, width), lambda i: (0, i))],
        out_specs=pl.BlockSpec((tokens, width), lambda i: (0, i)),
        scratch_shapes=[pltpu.VMEM((tokens, cells), jnp.bfloat16)],
    )(expert, slot, gate, r)


def solution(mesh):
    members = mesh.shape["ep"]

    def step(x, expert, slot, gate, w_gate, w_up, w_down):
        x, expert, slot, gate = x[0, 0], expert[0, 0].T, slot[0, 0].T, gate[0, 0].T
        (top, tokens), experts = expert.shape, members * w_gate.shape[0]
        slots = 5 * tokens * top // (4 * experts)
        r = moe(expert, slot, x, w_gate, w_up, w_down, members, slots)
        return combine(expert, slot, gate, r.reshape(experts * slots, x.shape[1]), slots)[None, None]

    own, weights = P("dp", "ep"), P("ep")
    return jax.shard_map(
        step, mesh=mesh, in_specs=(own, own, own, own, weights, weights, weights), out_specs=own, check_vma=False
    )
```

```python
import functools

import jax
import jax.numpy as jnp
from jax import lax
from jax.experimental import pallas as pl
from jax.experimental.pallas import tpu as pltpu
from jax.sharding import PartitionSpec as P

MESH = pl.DeviceIdType.MESH
FT, DT, RING, PAIR = 256, 512, 5, 2
AHEAD = RING - PAIR
CHUNKS, GROUP = 4, 4


def cell_of(expert_ref, slot_ref, slots):
    slot = slot_ref[...]
    return jnp.where(slot < slots, expert_ref[...] * slots + slot, -1)


def ffn_kernel(
    expert_ref, slot_ref, x_ref, wg, wu, wd, r_ref, sent, z, h, acc, ring,
    x_sem, w_sem, z_send, z_recv, c_send, c_recv, o_send, o_recv, o_own,
):
    experts, rows_z, d = z.shape
    members = r_ref.shape[0]
    slots = rows_z // members
    tokens, f = x_ref.shape[0], wg.shape[2]
    n1, n2 = f // FT, d // DT
    steps, total, back = n1 + n2, experts * (n1 + n2), n2 // PAIR
    me, group = lax.axis_index("ep"), lax.axis_index("dp")
    depth, early = d // CHUNKS, acc.shape[0]
    starts = CHUNKS * early // GROUP

    def peer(k):
        return me ^ k

    def rows(i):
        return pl.ds(pl.multiple_of(i * slots, slots), slots)

    def x_copy(j):
        return pltpu.make_async_copy(
            x_ref.at[:, pl.ds(j * DT, DT)], ring.at[RING - 1, pl.ds(j * tokens, tokens)], x_sem.at[j]
        )

    def w_issue(g):
        e, s, at = g // steps, lax.rem(g, steps), lax.rem(g, RING)

        @pl.when(g < starts)
        def _():
            q, m = g // (early // GROUP), lax.rem(g, early // GROUP)
            for i in range(GROUP):
                c = pl.ds(pl.multiple_of((m * GROUP + i) * FT, FT), FT)
                for j, w in enumerate((wg, wu)):
                    pltpu.make_async_copy(
                        w.at[0, pl.ds(pl.multiple_of(q * depth, depth), depth), c],
                        ring.at[at, pl.ds(i * depth, depth), pl.ds(j * FT, FT)],
                        w_sem.at[at, j],
                    ).start()

        @pl.when((s < n1) & (g < total) & (g >= starts))
        def _():
            c = pl.ds(pl.multiple_of(s * FT, FT), FT)
            for j, w in enumerate((wg, wu)):
                pltpu.make_async_copy(
                    w.at[e, :, c], ring.at[at, pl.ds(0, d), pl.ds(j * FT, FT)], w_sem.at[at, j]
                ).start()

        @pl.when((s >= n1) & (g < total))
        def _():
            c = pl.ds(pl.multiple_of((s - n1) * DT, DT), DT)
            pltpu.make_async_copy(wd.at[e, :, c], ring.at[at], w_sem.at[at, 0]).start()

    def z_copy(e, k):
        return pltpu.make_async_remote_copy(
            sent.at[e, pl.ds((k - 1) * slots, slots)], z.at[e, rows(me)], z_send.at[e, k - 1], z_recv.at[e, k - 1],
            device_id=(group, peer(k)), device_id_type=MESH,
        )

    def chunk_copy(q, k):
        c = pl.ds(pl.multiple_of(q * depth, depth), depth)
        return pltpu.make_async_remote_copy(
            sent.at[0, pl.ds((k - 1) * slots, slots), c], z.at[0, rows(me), c], c_send.at[q, k - 1],
            c_recv.at[q, k - 1], device_id=(group, peer(k)), device_id_type=MESH,
        )

    def chunk_arrival(q, k):
        c = pl.ds(pl.multiple_of(q * depth, depth), depth)
        return pltpu.make_async_remote_copy(
            sent.at[0, pl.ds((k - 1) * slots, slots), c], z.at[0, rows(peer(k)), c], c_send.at[q, k - 1],
            c_recv.at[q, k - 1], device_id=(group, peer(k)), device_id_type=MESH,
        )

    def z_arrival(e, k):
        return pltpu.make_async_remote_copy(
            sent.at[e, pl.ds((k - 1) * slots, slots)], z.at[e, rows(peer(k))], z_send.at[e, k - 1],
            z_recv.at[e, k - 1], device_id=(group, peer(k)), device_id_type=MESH,
        )

    def back_columns(s):
        return pl.ds(pl.multiple_of(s * (PAIR * DT), PAIR * DT), PAIR * DT)

    def o_copy(e, s, k):
        c = back_columns(s)
        return pltpu.make_async_remote_copy(
            z.at[e, rows(peer(k)), c], r_ref.at[me, e, :, c], o_send.at[e, s, k - 1],
            o_recv.at[e, s, k - 1], device_id=(group, peer(k)), device_id_type=MESH,
        )

    def o_arrival(e, s, k):
        c = back_columns(s)
        return pltpu.make_async_remote_copy(
            z.at[e, rows(me), c], r_ref.at[peer(k), e, :, c], o_send.at[e, s, k - 1],
            o_recv.at[e, s, k - 1], device_id=(group, peer(k)), device_id_type=MESH,
        )

    def o_local(e, s):
        c = back_columns(s)
        return pltpu.make_async_copy(z.at[e, rows(me), c], r_ref.at[me, e, :, c], o_own.at[e, s])

    for j in range(n2):
        x_copy(j).start()
    barrier = pltpu.get_barrier_semaphore()
    for k in (1, 2, 3):
        pl.semaphore_signal(barrier, inc=1, device_id=(group, peer(k)), device_id_type=MESH)
    for g in range(AHEAD):
        w_issue(jnp.int32(g))

    cell = cell_of(expert_ref, slot_ref, slots)
    row = lax.broadcasted_iota(jnp.int32, (rows_z, 1), 0)
    k_of = sum((row >= i * slots).astype(jnp.int32) for i in range(1, members))
    first = (me ^ k_of) * (experts * slots) + row - k_of * slots
    for j in range(n2):
        x_copy(j).wait()
    pl.semaphore_wait(barrier, 3)

    def send(e):
        for k in (2, 3, 1):
            z_copy(e, k).start()

    def send_chunk(q):
        for k in (2, 3, 1):
            chunk_copy(q, k).start()

    def dispatch(e, _):
        want = first + e * slots
        hot = ((cell[0:1] == want) | (cell[1:2] == want)).astype(jnp.float32).astype(z.dtype)

        def part(i, _):
            for j in range(PAIR):
                c = i * PAIR + j
                block = ring[RING - 1, pl.ds(pl.multiple_of(c * tokens, tokens), tokens), :]
                v = jnp.dot(hot, block, preferred_element_type=jnp.float32).astype(z.dtype)
                cols = pl.ds(pl.multiple_of(c * DT, DT), DT)
                z[e, rows(me), cols] = v[:slots]
                sent[e, :, cols] = v[slots:]

            @pl.when((e == 0) & (i > 0))
            def _():
                send_chunk(i - 1)

            @pl.when((e == 1) & (i == 0))
            def _():
                send_chunk(back - 1)

            @pl.when((e > 1) & (i == 0))
            def _():
                send(e - 1)

            return 0

        return lax.fori_loop(0, back, part, 0)

    lax.fori_loop(0, experts, dispatch, 0)

    def give_back(e, s):
        for k in (2, 3, 1):
            o_copy(e, s, k).start()
        o_local(e, s).start()

    def given(e):
        def one(s, _):
            for k in (1, 2, 3):
                o_copy(e, s, k).wait_send()
            o_local(e, s).wait()
            return 0

        lax.fori_loop(0, back, one, 0)

    def up_wait(at):
        for j, w in enumerate((wg, wu)):
            pltpu.make_async_copy(
                w.at[0, :, pl.ds(0, FT)], ring.at[at, pl.ds(0, d), pl.ds(j * FT, FT)], w_sem.at[at, j]
            ).wait()

    def start_step(final, g, _):
        q, m = g // (early // GROUP), lax.rem(g, early // GROUP)

        @pl.when(m == 0)
        def _():
            for k in (1, 2, 3):
                chunk_arrival(q, k).wait_recv()

        at = lax.rem(g, RING)
        w_issue(g + AHEAD)
        up_wait(at)
        c = pl.ds(pl.multiple_of(q * depth, depth), depth)
        for i in range(GROUP):
            t = m * GROUP + i
            w = ring[at, i * depth : (i + 1) * depth, :]
            both = acc[t] + jnp.dot(z[0, :, c], w, preferred_element_type=jnp.float32)
            if final:
                a, b = both[:, :FT], both[:, FT:]
                h[:, pl.ds(pl.multiple_of(t * FT, FT), FT)] = (jax.nn.silu(a) * b).astype(h.dtype)
            else:
                acc[t] = both
        return 0

    def up(e, s, n):
        g = e * steps + s
        for i in range(n):
            w_issue(g + AHEAD + i)
        for i in range(n):
            up_wait(lax.rem(g + i, RING))
        for i in range(n):
            both = jnp.dot(z[e], ring[lax.rem(g + i, RING), :d, :], preferred_element_type=jnp.float32)
            a, b = both[:, :FT], both[:, FT:]
            h[:, pl.ds(pl.multiple_of((s + i) * FT, FT), FT)] = (jax.nn.silu(a) * b).astype(h.dtype)

    def down(e, s, n):
        g = e * steps + n1 + s
        for i in range(n):
            w_issue(g + AHEAD + i)
        for i in range(n):
            at = lax.rem(g + i, RING)
            pltpu.make_async_copy(wd.at[0, :, pl.ds(0, DT)], ring.at[at], w_sem.at[at, 0]).wait()

        @pl.when(s > 0)
        def _():
            give_back(e, s // PAIR - 1)

        for i in range(n):
            c = pl.ds(pl.multiple_of((s + i) * DT, DT), DT)
            z[e, :, c] = jnp.dot(
                h[...], ring[lax.rem(g + i, RING)], preferred_element_type=jnp.float32
            ).astype(z.dtype)

    def in_pairs(step, e, done, n):
        def one(i, _):
            step(e, i * PAIR, PAIR)
            return 0

        lax.fori_loop(done // PAIR, n // PAIR, one, 0)
        if n % PAIR:
            step(e, n - n % PAIR, n % PAIR)

    def expert(e, _):
        @pl.when(e > 0)
        def _():
            for k in (1, 2, 3):
                z_arrival(e, k).wait_recv()
            give_back(e - 1, back - 1)

        in_pairs(up, e, early * (1 - (e + experts - 1) // experts), n1)
        in_pairs(down, e, 0, n2)
        return 0

    def clear(t, _):
        acc[t] = jnp.zeros(acc.shape[1:], acc.dtype)
        return 0

    lax.fori_loop(0, early, clear, 0)
    send(experts - 1)
    lax.fori_loop(0, starts - early // GROUP, functools.partial(start_step, False), 0)
    lax.fori_loop(starts - early // GROUP, starts, functools.partial(start_step, True), 0)
    lax.fori_loop(0, experts, expert, 0)
    for e in range(experts - 1):
        given(e)
    give_back(experts - 1, back - 1)
    given(experts - 1)
    for q in range(CHUNKS):
        for k in (1, 2, 3):
            chunk_copy(q, k).wait_send()

    def last(e, _):
        @pl.when(e > 0)
        def _():
            for k in (1, 2, 3):
                z_copy(e, k).wait_send()

        def one(s, _):
            for k in (1, 2, 3):
                o_arrival(e, s, k).wait_recv()
            return 0

        return lax.fori_loop(0, back, one, 0)

    lax.fori_loop(0, experts, last, 0)


def moe(expert, slot, x, wg, wu, wd, members, slots):
    experts, d, f = wg.shape
    back, dma, rows = d // (DT * PAIR), pltpu.SemaphoreType.DMA, members * slots
    n_early = GROUP * 3
    vmem, anywhere = pl.BlockSpec(memory_space=pltpu.VMEM), pl.BlockSpec(memory_space=pl.ANY)
    return pl.pallas_call(
        ffn_kernel,
        out_shape=jax.ShapeDtypeStruct((members, experts, slots, d), x.dtype),
        in_specs=[vmem, vmem] + [anywhere] * 4,
        out_specs=anywhere,
        scratch_shapes=[
            pltpu.VMEM((experts, rows - slots, d), x.dtype),
            pltpu.VMEM((experts, rows, d), x.dtype),
            pltpu.VMEM((rows, f), x.dtype),
            pltpu.VMEM((n_early, rows, 2 * FT), jnp.float32),
            pltpu.VMEM((RING, f, 2 * FT), x.dtype),
            dma((d // DT,)),
            dma((RING, 2)),
            dma((experts, 3)),
            dma((experts, 3)),
            dma((CHUNKS, 3)),
            dma((CHUNKS, 3)),
            dma((experts, back, 3)),
            dma((experts, back, 3)),
            dma((experts, back)),
        ],
        compiler_params=pltpu.CompilerParams(
            collective_id=0, has_side_effects=True, vmem_limit_bytes=67_000_000
        ),
    )(expert, slot, x, wg, wu, wd)


def combine_kernel(expert_ref, slot_ref, gate_ref, r_ref, y_ref, weights, *, slots):
    @pl.when(pl.program_id(0) == 0)
    def _():
        cell, gate = cell_of(expert_ref, slot_ref, slots), gate_ref[...].astype(jnp.bfloat16).astype(jnp.float32)
        top = cell.shape[0]
        both = jnp.concatenate([cell.astype(jnp.float32), gate] * (4 // top), axis=0).T
        q = lax.broadcasted_iota(jnp.int32, weights.shape, 1).astype(jnp.float32)
        w = sum(jnp.where(both[:, j : j + 1] == q, both[:, top + j : top + j + 1], 0.0) for j in range(top))
        weights[...] = w.astype(jnp.bfloat16)

    y_ref[...] = jnp.dot(weights[...], r_ref[...], preferred_element_type=jnp.float32).astype(y_ref.dtype)


def combine(expert, slot, gate, r, slots):
    (top, tokens), (cells, d), width = expert.shape, r.shape, 512
    small = pl.BlockSpec((top, tokens), lambda i: (0, 0))
    return pl.pallas_call(
        functools.partial(combine_kernel, slots=slots),
        out_shape=jax.ShapeDtypeStruct((tokens, d), jnp.bfloat16),
        grid=(d // width,),
        in_specs=[small, small, small, pl.BlockSpec((cells, width), lambda i: (0, i))],
        out_specs=pl.BlockSpec((tokens, width), lambda i: (0, i)),
        scratch_shapes=[pltpu.VMEM((tokens, cells), jnp.bfloat16)],
    )(expert, slot, gate, r)


def solution(mesh):
    members = mesh.shape["ep"]

    def step(x, expert, slot, gate, w_gate, w_up, w_down):
        x, expert, slot, gate = x[0, 0], expert[0, 0].T, slot[0, 0].T, gate[0, 0].T
        (top, tokens), experts = expert.shape, members * w_gate.shape[0]
        slots = 5 * tokens * top // (4 * experts)
        r = moe(expert, slot, x, w_gate, w_up, w_down, members, slots)
        return combine(expert, slot, gate, r.reshape(experts * slots, x.shape[1]), slots)[None, None]

    own, weights = P("dp", "ep"), P("ep")
    return jax.shard_map(
        step, mesh=mesh, in_specs=(own, own, own, own, weights, weights, weights), out_specs=own, check_vma=False
    )
```

```python
import functools

import jax
import jax.numpy as jnp
from jax import lax
from jax.experimental import pallas as pl
from jax.experimental.pallas import tpu as pltpu
from jax.sharding import PartitionSpec as P

MESH = pl.DeviceIdType.MESH
FT, DT, RING, PAIR = 256, 512, 5, 2
AHEAD = RING - PAIR
CHUNKS, GROUP = 4, 4


def cell_of(expert_ref, slot_ref, slots):
    slot = slot_ref[...]
    return jnp.where(slot < slots, expert_ref[...] * slots + slot, -1)


def ffn_kernel(
    expert_ref, slot_ref, gate_ref, x_ref, wg, wu, wd, y_ref, r_ref, sent, z, h, acc, ring, weights,
    x_sem, w_sem, z_send, z_recv, c_send, c_recv, o_send, o_recv, o_own, r_sem, y_sem,
):
    experts, rows_z, d = z.shape
    members = r_ref.shape[0]
    slots = rows_z // members
    tokens, f = x_ref.shape[0], wg.shape[2]
    n1, n2 = f // FT, d // DT
    steps, total, back = n1 + n2, experts * (n1 + n2), n2 // PAIR
    me, group = lax.axis_index("ep"), lax.axis_index("dp")
    depth, early = d // CHUNKS, acc.shape[0]
    starts = CHUNKS * early // GROUP

    def peer(k):
        return me ^ k

    def rows(i):
        return pl.ds(pl.multiple_of(i * slots, slots), slots)

    def x_copy(j):
        return pltpu.make_async_copy(
            x_ref.at[:, pl.ds(j * DT, DT)], ring.at[RING - 1, pl.ds(j * tokens, tokens)], x_sem.at[j]
        )

    def w_issue(g):
        e, s, at = g // steps, lax.rem(g, steps), lax.rem(g, RING)

        @pl.when(g < starts)
        def _():
            q, m = g // (early // GROUP), lax.rem(g, early // GROUP)
            for i in range(GROUP):
                c = pl.ds(pl.multiple_of((m * GROUP + i) * FT, FT), FT)
                for j, w in enumerate((wg, wu)):
                    pltpu.make_async_copy(
                        w.at[0, pl.ds(pl.multiple_of(q * depth, depth), depth), c],
                        ring.at[at, pl.ds(i * depth, depth), pl.ds(j * FT, FT)],
                        w_sem.at[at, j],
                    ).start()

        @pl.when((s < n1) & (g < total) & (g >= starts))
        def _():
            c = pl.ds(pl.multiple_of(s * FT, FT), FT)
            for j, w in enumerate((wg, wu)):
                pltpu.make_async_copy(
                    w.at[e, :, c], ring.at[at, pl.ds(0, d), pl.ds(j * FT, FT)], w_sem.at[at, j]
                ).start()

        @pl.when((s >= n1) & (g < total))
        def _():
            c = pl.ds(pl.multiple_of((s - n1) * DT, DT), DT)
            pltpu.make_async_copy(wd.at[e, :, c], ring.at[at], w_sem.at[at, 0]).start()

    def z_copy(e, k):
        return pltpu.make_async_remote_copy(
            sent.at[e, pl.ds((k - 1) * slots, slots)], z.at[e, rows(me)], z_send.at[e, k - 1], z_recv.at[e, k - 1],
            device_id=(group, peer(k)), device_id_type=MESH,
        )

    def chunk_copy(q, k):
        c = pl.ds(pl.multiple_of(q * depth, depth), depth)
        return pltpu.make_async_remote_copy(
            sent.at[0, pl.ds((k - 1) * slots, slots), c], z.at[0, rows(me), c], c_send.at[q, k - 1],
            c_recv.at[q, k - 1], device_id=(group, peer(k)), device_id_type=MESH,
        )

    def chunk_arrival(q, k):
        c = pl.ds(pl.multiple_of(q * depth, depth), depth)
        return pltpu.make_async_remote_copy(
            sent.at[0, pl.ds((k - 1) * slots, slots), c], z.at[0, rows(peer(k)), c], c_send.at[q, k - 1],
            c_recv.at[q, k - 1], device_id=(group, peer(k)), device_id_type=MESH,
        )

    def z_arrival(e, k):
        return pltpu.make_async_remote_copy(
            sent.at[e, pl.ds((k - 1) * slots, slots)], z.at[e, rows(peer(k))], z_send.at[e, k - 1],
            z_recv.at[e, k - 1], device_id=(group, peer(k)), device_id_type=MESH,
        )

    def back_columns(s):
        return pl.ds(pl.multiple_of(s * (PAIR * DT), PAIR * DT), PAIR * DT)

    def o_copy(e, s, k):
        c = back_columns(s)
        return pltpu.make_async_remote_copy(
            z.at[e, rows(peer(k)), c], r_ref.at[me, rows(e), c], o_send.at[e, s, k - 1],
            o_recv.at[e, s, k - 1], device_id=(group, peer(k)), device_id_type=MESH,
        )

    def o_arrival(e, s, k):
        c = back_columns(s)
        return pltpu.make_async_remote_copy(
            z.at[e, rows(me), c], r_ref.at[peer(k), rows(e), c], o_send.at[e, s, k - 1],
            o_recv.at[e, s, k - 1], device_id=(group, peer(k)), device_id_type=MESH,
        )

    def o_local(e, s):
        c = back_columns(s)
        return pltpu.make_async_copy(z.at[e, rows(me), c], r_ref.at[me, rows(e), c], o_own.at[e, s])

    for j in range(n2):
        x_copy(j).start()
    barrier = pltpu.get_barrier_semaphore()
    for k in (1, 2, 3):
        pl.semaphore_signal(barrier, inc=1, device_id=(group, peer(k)), device_id_type=MESH)
    for g in range(AHEAD):
        w_issue(jnp.int32(g))

    cell = cell_of(expert_ref, slot_ref, slots)
    row = lax.broadcasted_iota(jnp.int32, (rows_z, 1), 0)
    k_of = sum((row >= i * slots).astype(jnp.int32) for i in range(1, members))
    first = (me ^ k_of) * (experts * slots) + row - k_of * slots
    for j in range(n2):
        x_copy(j).wait()
    pl.semaphore_wait(barrier, 3)

    def send(e):
        for k in (2, 3, 1):
            z_copy(e, k).start()

    def send_chunk(q):
        for k in (2, 3, 1):
            chunk_copy(q, k).start()

    def dispatch(e, _):
        want = first + e * slots
        hot = ((cell[0:1] == want) | (cell[1:2] == want)).astype(jnp.float32).astype(z.dtype)

        def part(i, _):
            for j in range(PAIR):
                c = i * PAIR + j
                block = ring[RING - 1, pl.ds(pl.multiple_of(c * tokens, tokens), tokens), :]
                v = jnp.dot(hot, block, preferred_element_type=jnp.float32).astype(z.dtype)
                cols = pl.ds(pl.multiple_of(c * DT, DT), DT)
                z[e, rows(me), cols] = v[:slots]
                sent[e, :, cols] = v[slots:]

            @pl.when((e == 0) & (i > 0))
            def _():
                send_chunk(i - 1)

            @pl.when((e == 1) & (i == 0))
            def _():
                send_chunk(back - 1)

            @pl.when((e > 1) & (i == 0))
            def _():
                send(e - 1)

            return 0

        return lax.fori_loop(0, back, part, 0)

    lax.fori_loop(0, experts, dispatch, 0)

    def give_back(e, s):
        for k in (2, 3, 1):
            o_copy(e, s, k).start()
        o_local(e, s).start()

    def up_wait(at):
        for j, w in enumerate((wg, wu)):
            pltpu.make_async_copy(
                w.at[0, :, pl.ds(0, FT)], ring.at[at, pl.ds(0, d), pl.ds(j * FT, FT)], w_sem.at[at, j]
            ).wait()

    def start_step(final, g, _):
        q, m = g // (early // GROUP), lax.rem(g, early // GROUP)

        @pl.when(m == 0)
        def _():
            for k in (1, 2, 3):
                chunk_arrival(q, k).wait_recv()

        at = lax.rem(g, RING)
        w_issue(g + AHEAD)
        up_wait(at)
        c = pl.ds(pl.multiple_of(q * depth, depth), depth)
        for i in range(GROUP):
            t = m * GROUP + i
            w = ring[at, i * depth : (i + 1) * depth, :]
            both = acc[t] + jnp.dot(z[0, :, c], w, preferred_element_type=jnp.float32)
            if final:
                a, b = both[:, :FT], both[:, FT:]
                h[:, pl.ds(pl.multiple_of(t * FT, FT), FT)] = (jax.nn.silu(a) * b).astype(h.dtype)
            else:
                acc[t] = both
        return 0

    def up(e, s, n):
        g = e * steps + s
        for i in range(n):
            w_issue(g + AHEAD + i)
        for i in range(n):
            up_wait(lax.rem(g + i, RING))
        for i in range(n):
            both = jnp.dot(z[e], ring[lax.rem(g + i, RING), :d, :], preferred_element_type=jnp.float32)
            a, b = both[:, :FT], both[:, FT:]
            h[:, pl.ds(pl.multiple_of((s + i) * FT, FT), FT)] = (jax.nn.silu(a) * b).astype(h.dtype)

    def down(e, s, n):
        g = e * steps + n1 + s
        for i in range(n):
            w_issue(g + AHEAD + i)
        for i in range(n):
            at = lax.rem(g + i, RING)
            pltpu.make_async_copy(wd.at[0, :, pl.ds(0, DT)], ring.at[at], w_sem.at[at, 0]).wait()

        @pl.when(s > 0)
        def _():
            give_back(e, s // PAIR - 1)

        for i in range(n):
            c = pl.ds(pl.multiple_of((s + i) * DT, DT), DT)
            z[e, :, c] = jnp.dot(
                h[...], ring[lax.rem(g + i, RING)], preferred_element_type=jnp.float32
            ).astype(z.dtype)

    def in_pairs(step, e, done, n):
        def one(i, _):
            step(e, i * PAIR, PAIR)
            return 0

        lax.fori_loop(done // PAIR, n // PAIR, one, 0)
        if n % PAIR:
            step(e, n - n % PAIR, n % PAIR)

    def expert(e, _):
        @pl.when(e > 0)
        def _():
            for k in (1, 2, 3):
                z_arrival(e, k).wait_recv()
            give_back(e - 1, back - 1)

        in_pairs(up, e, early * (1 - (e + experts - 1) // experts), n1)
        in_pairs(down, e, 0, n2)
        return 0

    def clear(t, _):
        acc[t] = jnp.zeros(acc.shape[1:], acc.dtype)
        return 0

    lax.fori_loop(0, early, clear, 0)
    send(experts - 1)
    top = cell.shape[0]
    gate = gate_ref[...].astype(jnp.bfloat16).astype(jnp.float32)
    both = jnp.concatenate([cell.astype(jnp.float32), gate] * (4 // top), axis=0).T

    def weigh(i, _):
        c = pl.ds(pl.multiple_of(i * 256, 256), 256)
        q = (lax.broadcasted_iota(jnp.int32, (tokens, 256), 1) + i * 256).astype(jnp.float32)
        w = sum(jnp.where(both[:, j : j + 1] == q, both[:, top + j : top + j + 1], 0.0) for j in range(top))
        weights[:, c] = w.astype(weights.dtype)
        return 0

    lax.fori_loop(0, weights.shape[1] // 256, weigh, 0)
    lax.fori_loop(0, starts - early // GROUP, functools.partial(start_step, False), 0)
    lax.fori_loop(starts - early // GROUP, starts, functools.partial(start_step, True), 0)
    lax.fori_loop(0, experts, expert, 0)
    give_back(experts - 1, back - 1)

    cells, per = members * rows_z, f // (members * rows_z)

    def r_copy(c, i):
        return pltpu.make_async_copy(
            r_ref.at[i, :, pl.ds(pl.multiple_of(c * DT, DT), DT)],
            ring.at[c // per, pl.ds(pl.multiple_of(lax.rem(c, per) * cells + i * rows_z, rows_z), rows_z)],
            r_sem.at[c, i],
        )

    def y_copy(c):
        return pltpu.make_async_copy(
            ring.at[2, pl.ds(pl.multiple_of(c * tokens, tokens), tokens)],
            y_ref.at[:, pl.ds(pl.multiple_of(c * DT, DT), DT)],
            y_sem.at[c],
        )

    def arrived(s):
        def one(e, _):
            for k in (1, 2, 3):
                o_arrival(e, s, k).wait_recv()
            o_local(e, s).wait()
            return 0

        lax.fori_loop(0, experts, one, 0)

    def merge(s, _):
        arrived(s)
        for j in range(PAIR):
            for i in range(members):
                r_copy(s * PAIR + j, i).start()
        for j in range(PAIR):
            for i in range(members):
                r_copy(s * PAIR + j, i).wait()
        for j in range(PAIR):
            c = s * PAIR + j
            block = ring[c // per, pl.ds(pl.multiple_of(lax.rem(c, per) * cells, cells), cells), :]
            v = jnp.dot(weights[...], block, preferred_element_type=jnp.float32)
            ring[2, pl.ds(pl.multiple_of(c * tokens, tokens), tokens), :] = v.astype(ring.dtype)
        for j in range(PAIR):
            y_copy(s * PAIR + j).start()
        return 0

    lax.fori_loop(0, back, merge, 0)
    for q in range(CHUNKS):
        for k in (1, 2, 3):
            chunk_copy(q, k).wait_send()

    def last(e, _):
        @pl.when(e > 0)
        def _():
            for k in (1, 2, 3):
                z_copy(e, k).wait_send()

        def one(s, _):
            for k in (1, 2, 3):
                o_copy(e, s, k).wait_send()
            return 0

        return lax.fori_loop(0, back, one, 0)

    lax.fori_loop(0, experts, last, 0)

    def written(c, _):
        y_copy(c).wait()
        return 0

    lax.fori_loop(0, n2, written, 0)


def moe(expert, slot, gate, x, wg, wu, wd, members, slots):
    experts, d, f = wg.shape
    back, dma, rows = d // (DT * PAIR), pltpu.SemaphoreType.DMA, members * slots
    n_early = GROUP * 3
    vmem, anywhere = pl.BlockSpec(memory_space=pltpu.VMEM), pl.BlockSpec(memory_space=pl.ANY)
    return pl.pallas_call(
        ffn_kernel,
        out_shape=(
            jax.ShapeDtypeStruct(x.shape, x.dtype),
            jax.ShapeDtypeStruct((members, rows, d), x.dtype),
        ),
        in_specs=[vmem] * 3 + [anywhere] * 4,
        out_specs=(anywhere, anywhere),
        scratch_shapes=[
            pltpu.VMEM((experts, rows - slots, d), x.dtype),
            pltpu.VMEM((experts, rows, d), x.dtype),
            pltpu.VMEM((rows, f), x.dtype),
            pltpu.VMEM((n_early, rows, 2 * FT), jnp.float32),
            pltpu.VMEM((RING, f, 2 * FT), x.dtype),
            pltpu.VMEM((x.shape[0], members * rows), x.dtype),
            dma((d // DT,)),
            dma((RING, 2)),
            dma((experts, 3)),
            dma((experts, 3)),
            dma((CHUNKS, 3)),
            dma((CHUNKS, 3)),
            dma((experts, back, 3)),
            dma((experts, back, 3)),
            dma((experts, back)),
            dma((d // DT, members)),
            dma((d // DT,)),
        ],
        compiler_params=pltpu.CompilerParams(
            collective_id=0, has_side_effects=True, vmem_limit_bytes=67_000_000
        ),
    )(expert, slot, gate, x, wg, wu, wd)[0]


def solution(mesh):
    members = mesh.shape["ep"]

    def step(x, expert, slot, gate, w_gate, w_up, w_down):
        x, expert, slot, gate = x[0, 0], expert[0, 0].T, slot[0, 0].T, gate[0, 0].T
        (top, tokens), experts = expert.shape, members * w_gate.shape[0]
        slots = 5 * tokens * top // (4 * experts)
        return moe(expert, slot, gate, x, w_gate, w_up, w_down, members, slots)[None, None]

    own, weights = P("dp", "ep"), P("ep")
    return jax.shard_map(
        step, mesh=mesh, in_specs=(own, own, own, own, weights, weights, weights), out_specs=own, check_vma=False
    )
```

```python
import functools

import jax
import jax.numpy as jnp
from jax import lax
from jax.experimental import pallas as pl
from jax.experimental.pallas import tpu as pltpu
from jax.sharding import PartitionSpec as P

MESH = pl.DeviceIdType.MESH
FT, DT, RING, PAIR = 256, 512, 5, 2
AHEAD = RING - PAIR
CHUNKS, GROUP = 4, 4


def cell_of(expert_ref, slot_ref, slots):
    slot = slot_ref[...]
    return jnp.where(slot < slots, expert_ref[...] * slots + slot, -1)


def ffn_kernel(
    expert_ref, slot_ref, gate_ref, x_ref, wg, wu, wd, y_ref, r_ref, sent, z, h, acc, ring,
    x_sem, w_sem, z_send, z_recv, c_send, c_recv, o_send, o_recv, o_own, r_sem, y_sem, free,
):
    experts, rows_z, d = z.shape
    members = r_ref.shape[0]
    slots = rows_z // members
    tokens, f = x_ref.shape[0], wg.shape[2]
    n1, n2 = f // FT, d // DT
    steps, total, back = n1 + n2, experts * (n1 + n2), n2 // PAIR
    me, group = lax.axis_index("ep"), lax.axis_index("dp")
    depth, early = d // CHUNKS, acc.shape[0]
    starts = CHUNKS * early // GROUP

    def peer(k):
        return me ^ k

    def rows(i):
        return pl.ds(pl.multiple_of(i * slots, slots), slots)

    def x_copy(j):
        return pltpu.make_async_copy(
            x_ref.at[:, pl.ds(pl.multiple_of(j * DT, DT), DT)],
            ring.at[RING - 1, pl.ds(pl.multiple_of(j * tokens, tokens), tokens)],
            x_sem.at[j],
        )

    def w_issue(g):
        e, s, at = g // steps, lax.rem(g, steps), lax.rem(g, RING)

        @pl.when(g < starts)
        def _():
            q, m = g // (early // GROUP), lax.rem(g, early // GROUP)
            for i in range(GROUP):
                c = pl.ds(pl.multiple_of((m * GROUP + i) * FT, FT), FT)
                for j, w in enumerate((wg, wu)):
                    pltpu.make_async_copy(
                        w.at[0, pl.ds(pl.multiple_of(q * depth, depth), depth), c],
                        ring.at[at, pl.ds(i * depth, depth), pl.ds(j * FT, FT)],
                        w_sem.at[at, j],
                    ).start()

        @pl.when((s < n1) & (g < total) & (g >= starts))
        def _():
            c = pl.ds(pl.multiple_of(s * FT, FT), FT)
            for j, w in enumerate((wg, wu)):
                pltpu.make_async_copy(
                    w.at[e, :, c], ring.at[at, pl.ds(0, d), pl.ds(j * FT, FT)], w_sem.at[at, j]
                ).start()

        @pl.when((s >= n1) & (g < total))
        def _():
            c = pl.ds(pl.multiple_of((s - n1) * DT, DT), DT)
            pltpu.make_async_copy(wd.at[e, :, c], ring.at[at], w_sem.at[at, 0]).start()

    def z_copy(e, k):
        return pltpu.make_async_remote_copy(
            sent.at[e - 1, pl.ds((k - 1) * slots, slots)], z.at[e, rows(me)], z_send.at[e, k - 1], z_recv.at[e, k - 1],
            device_id=(group, peer(k)), device_id_type=MESH,
        )

    def chunk_copy(q, k):
        c = pl.ds(pl.multiple_of(q * depth, depth), depth)
        return pltpu.make_async_remote_copy(
            z.at[experts - 1, rows(peer(k)), c], z.at[0, rows(me), c], c_send.at[q, k - 1],
            c_recv.at[q, k - 1], device_id=(group, peer(k)), device_id_type=MESH,
        )

    def chunk_arrival(q, k):
        c = pl.ds(pl.multiple_of(q * depth, depth), depth)
        return pltpu.make_async_remote_copy(
            z.at[experts - 1, rows(peer(k)), c], z.at[0, rows(peer(k)), c], c_send.at[q, k - 1],
            c_recv.at[q, k - 1], device_id=(group, peer(k)), device_id_type=MESH,
        )

    def z_arrival(e, k):
        return pltpu.make_async_remote_copy(
            sent.at[e - 1, pl.ds((k - 1) * slots, slots)], z.at[e, rows(peer(k))], z_send.at[e, k - 1],
            z_recv.at[e, k - 1], device_id=(group, peer(k)), device_id_type=MESH,
        )

    def back_columns(s):
        return pl.ds(pl.multiple_of(s * (PAIR * DT), PAIR * DT), PAIR * DT)

    def o_copy(e, s, k):
        c = back_columns(s)
        return pltpu.make_async_remote_copy(
            z.at[e, rows(peer(k)), c], r_ref.at[me, rows(e), c], o_send.at[e, s, k - 1],
            o_recv.at[e, s, k - 1], device_id=(group, peer(k)), device_id_type=MESH,
        )

    def o_arrival(e, s, k):
        c = back_columns(s)
        return pltpu.make_async_remote_copy(
            z.at[e, rows(me), c], r_ref.at[peer(k), rows(e), c], o_send.at[e, s, k - 1],
            o_recv.at[e, s, k - 1], device_id=(group, peer(k)), device_id_type=MESH,
        )

    def o_local(e, s):
        c = back_columns(s)
        return pltpu.make_async_copy(z.at[e, rows(me), c], r_ref.at[me, rows(e), c], o_own.at[e, s])

    for j in range(n2):
        x_copy(j).start()
    barrier = pltpu.get_barrier_semaphore()
    for k in (1, 2, 3):
        pl.semaphore_signal(barrier, inc=1, device_id=(group, peer(k)), device_id_type=MESH)

    cell = cell_of(expert_ref, slot_ref, slots)
    row = lax.broadcasted_iota(jnp.int32, (rows_z, 1), 0)
    k_of = sum((row >= i * slots).astype(jnp.int32) for i in range(1, members))
    first = (me ^ k_of) * (experts * slots) + row - k_of * slots
    pl.semaphore_wait(barrier, 3)

    def send(e):
        for k in (2, 3, 1):
            z_copy(e, k).start()

    def send_chunk(q):
        for k in (2, 3, 1):
            chunk_copy(q, k).start()

    def dispatch(e, _):
        want = first + e * slots
        hot = ((cell[0:1] == want) | (cell[1:2] == want)).astype(jnp.float32).astype(z.dtype)

        def part(i, _):
            @pl.when(e == 0)
            def _():
                for j in range(PAIR):
                    x_copy(i * PAIR + j).wait()

            @pl.when((e == 0) & (i == back - 1))
            def _():
                for g in range(AHEAD):
                    w_issue(jnp.int32(g))

            for j in range(PAIR):
                c = i * PAIR + j
                block = ring[RING - 1, pl.ds(pl.multiple_of(c * tokens, tokens), tokens), :]
                v = jnp.dot(hot, block, preferred_element_type=jnp.float32).astype(z.dtype)
                cols = pl.ds(pl.multiple_of(c * DT, DT), DT)
                z[e, rows(me), cols] = v[:slots]

                @pl.when(e == 0)
                def _():
                    for k in (1, 2, 3):
                        z[experts - 1, rows(peer(k)), cols] = v[k * slots : (k + 1) * slots]

                @pl.when(e > 0)
                def _():
                    sent[e - 1, :, cols] = v[slots:]

            @pl.when((e == 0) & (i > 0))
            def _():
                send_chunk(i - 1)

            @pl.when((e == 1) & (i == 0))
            def _():
                send_chunk(back - 1)

            @pl.when((e > 1) & (i == 0))
            def _():
                send(e - 1)

            return 0

        return lax.fori_loop(0, back, part, 0)

    lax.fori_loop(0, experts, dispatch, 0)

    def give_back(e, s):
        for k in (2, 3, 1):
            o_copy(e, s, k).start()
        o_local(e, s).start()

    def up_wait(at):
        for j, w in enumerate((wg, wu)):
            pltpu.make_async_copy(
                w.at[0, :, pl.ds(0, FT)], ring.at[at, pl.ds(0, d), pl.ds(j * FT, FT)], w_sem.at[at, j]
            ).wait()

    def start_step(final, g, _):
        q, m = g // (early // GROUP), lax.rem(g, early // GROUP)

        @pl.when(m == 0)
        def _():
            for k in (1, 2, 3):
                chunk_arrival(q, k).wait_recv()

        at = lax.rem(g, RING)
        w_issue(g + AHEAD)
        up_wait(at)
        c = pl.ds(pl.multiple_of(q * depth, depth), depth)
        for i in range(GROUP):
            t = m * GROUP + i
            w = ring[at, i * depth : (i + 1) * depth, :]
            both = acc[t] + jnp.dot(z[0, :, c], w, preferred_element_type=jnp.float32)
            if final:
                a, b = both[:, :FT], both[:, FT:]
                h[:, pl.ds(pl.multiple_of(t * FT, FT), FT)] = (jax.nn.silu(a) * b).astype(h.dtype)
            else:
                acc[t] = both
        return 0

    def up(e, s, n):
        g = e * steps + s
        for i in range(n):
            w_issue(g + AHEAD + i)
        for i in range(n):
            up_wait(lax.rem(g + i, RING))
        for i in range(n):
            both = jnp.dot(z[e], ring[lax.rem(g + i, RING), :d, :], preferred_element_type=jnp.float32)
            a, b = both[:, :FT], both[:, FT:]
            h[:, pl.ds(pl.multiple_of((s + i) * FT, FT), FT)] = (jax.nn.silu(a) * b).astype(h.dtype)

    def down(e, s, n):
        g = e * steps + n1 + s
        for i in range(n):
            w_issue(g + AHEAD + i)
        for i in range(n):
            at = lax.rem(g + i, RING)
            pltpu.make_async_copy(wd.at[0, :, pl.ds(0, DT)], ring.at[at], w_sem.at[at, 0]).wait()

        @pl.when(s > 0)
        def _():
            give_back(e, s // PAIR - 1)

        for i in range(n):
            c = pl.ds(pl.multiple_of((s + i) * DT, DT), DT)
            z[e, :, c] = jnp.dot(
                h[...], ring[lax.rem(g + i, RING)], preferred_element_type=jnp.float32
            ).astype(z.dtype)

    def in_pairs(step, e, done, n):
        def one(i, _):
            step(e, i * PAIR, PAIR)
            return 0

        lax.fori_loop(done // PAIR, n // PAIR, one, 0)
        if n % PAIR:
            step(e, n - n % PAIR, n % PAIR)

    def expert(e, _):
        @pl.when(e > 0)
        def _():
            for k in (1, 2, 3):
                z_arrival(e, k).wait_recv()
            give_back(e - 1, back - 1)

        in_pairs(up, e, early * (1 - (e + experts - 1) // experts), n1)

        @pl.when(e == 0)
        def _():
            pl.semaphore_wait(free, 3)
            send(experts - 1)

        in_pairs(down, e, 0, n2)
        return 0

    def clear(t, _):
        acc[t] = jnp.zeros(acc.shape[1:], acc.dtype)
        return 0

    lax.fori_loop(0, early, clear, 0)
    lax.fori_loop(0, starts - early // GROUP, functools.partial(start_step, False), 0)
    lax.fori_loop(starts - early // GROUP, starts, functools.partial(start_step, True), 0)
    for q in range(CHUNKS):
        for k in (1, 2, 3):
            chunk_copy(q, k).wait_send()
    for k in (1, 2, 3):
        pl.semaphore_signal(free, inc=1, device_id=(group, peer(k)), device_id_type=MESH)
    lax.fori_loop(0, experts, expert, 0)
    give_back(experts - 1, back - 1)

    cells, per = members * rows_z, f // (members * rows_z)
    top, half = cell.shape[0], DT // 2
    gate = gate_ref[...].astype(jnp.bfloat16).astype(jnp.float32)
    both = jnp.concatenate([cell_of(expert_ref, slot_ref, slots).astype(jnp.float32), gate] * (4 // top), axis=0).T
    for i in range(cells // half):
        q = (lax.broadcasted_iota(jnp.int32, (tokens, half), 1) + i * half).astype(jnp.float32)
        w = sum(jnp.where(both[:, j : j + 1] == q, both[:, top + j : top + j + 1], 0.0) for j in range(top))
        at = i // 2 * tokens
        ring[3, at : at + tokens, i % 2 * half : (i % 2 + 1) * half] = w.astype(ring.dtype)

    def weighted(c):
        v = 0.0
        for i in range(0, cells, DT):
            n, at = min(DT, cells - i), i // DT * tokens
            block = ring[c // per, pl.ds(pl.multiple_of(lax.rem(c, per) * cells + i, half), n), :]
            v += jnp.dot(ring[3, at : at + tokens, :n], block, preferred_element_type=jnp.float32)
        return v

    def r_copy(c, i):
        return pltpu.make_async_copy(
            r_ref.at[i, :, pl.ds(pl.multiple_of(c * DT, DT), DT)],
            ring.at[c // per, pl.ds(pl.multiple_of(lax.rem(c, per) * cells + i * rows_z, rows_z), rows_z)],
            r_sem.at[c, i],
        )

    def y_copy(c):
        return pltpu.make_async_copy(
            ring.at[2, pl.ds(pl.multiple_of(c * tokens, tokens), tokens)],
            y_ref.at[:, pl.ds(pl.multiple_of(c * DT, DT), DT)],
            y_sem.at[c],
        )

    def arrived(s):
        def one(e, _):
            for k in (1, 2, 3):
                o_arrival(e, s, k).wait_recv()
            o_local(e, s).wait()
            return 0

        lax.fori_loop(0, experts, one, 0)

    def merge(s, _):
        arrived(s)
        for j in range(PAIR):
            for i in range(members):
                r_copy(s * PAIR + j, i).start()
        for j in range(PAIR):
            for i in range(members):
                r_copy(s * PAIR + j, i).wait()
        for j in range(PAIR):
            c = s * PAIR + j
            ring[2, pl.ds(pl.multiple_of(c * tokens, tokens), tokens), :] = weighted(c).astype(ring.dtype)
        for j in range(PAIR):
            y_copy(s * PAIR + j).start()
        return 0

    lax.fori_loop(0, back, merge, 0)

    def last(e, _):
        @pl.when(e > 0)
        def _():
            for k in (1, 2, 3):
                z_copy(e, k).wait_send()

        def one(s, _):
            for k in (1, 2, 3):
                o_copy(e, s, k).wait_send()
            return 0

        return lax.fori_loop(0, back, one, 0)

    lax.fori_loop(0, experts, last, 0)

    def written(c, _):
        y_copy(c).wait()
        return 0

    lax.fori_loop(0, n2, written, 0)


def moe(expert, slot, gate, x, wg, wu, wd, members, slots):
    experts, d, f = wg.shape
    back, dma, rows = d // (DT * PAIR), pltpu.SemaphoreType.DMA, members * slots
    n_early = GROUP * 4
    vmem, anywhere = pl.BlockSpec(memory_space=pltpu.VMEM), pl.BlockSpec(memory_space=pl.ANY)
    return pl.pallas_call(
        ffn_kernel,
        out_shape=(
            jax.ShapeDtypeStruct(x.shape, x.dtype),
            jax.ShapeDtypeStruct((members, rows, d), x.dtype),
        ),
        in_specs=[vmem] * 3 + [anywhere] * 4,
        out_specs=(anywhere, anywhere),
        scratch_shapes=[
            pltpu.VMEM((experts - 1, rows - slots, d), x.dtype),
            pltpu.VMEM((experts, rows, d), x.dtype),
            pltpu.VMEM((rows, f), x.dtype),
            pltpu.VMEM((n_early, rows, 2 * FT), jnp.float32),
            pltpu.VMEM((RING, f, 2 * FT), x.dtype),
            dma((d // DT,)),
            dma((RING, 2)),
            dma((experts, 3)),
            dma((experts, 3)),
            dma((CHUNKS, 3)),
            dma((CHUNKS, 3)),
            dma((experts, back, 3)),
            dma((experts, back, 3)),
            dma((experts, back)),
            dma((d // DT, members)),
            dma((d // DT,)),
            pltpu.SemaphoreType.REGULAR,
        ],
        compiler_params=pltpu.CompilerParams(
            collective_id=0, has_side_effects=True, vmem_limit_bytes=67_000_000
        ),
    )(expert, slot, gate, x, wg, wu, wd)[0]


def solution(mesh):
    members = mesh.shape["ep"]

    def step(x, expert, slot, gate, w_gate, w_up, w_down):
        x, expert, slot, gate = x[0, 0], expert[0, 0].T, slot[0, 0].T, gate[0, 0].T
        (top, tokens), experts = expert.shape, members * w_gate.shape[0]
        slots = 5 * tokens * top // (4 * experts)
        return moe(expert, slot, gate, x, w_gate, w_up, w_down, members, slots)[None, None]

    own, weights = P("dp", "ep"), P("ep")
    return jax.shard_map(
        step, mesh=mesh, in_specs=(own, own, own, own, weights, weights, weights), out_specs=own, check_vma=False
    )
```
